32 devices in a mesh: gx: 4 (over z), gy: 4 (over y, x), gz: 2 (over core).
Axes of the slice: x: 2, y: 2, z: 4, core: 2. Of those that a mesh axis runs over, the one named last changes fastest.
Arguments:
- panel: float32 [8192, 4096], P(('gx', 'gy', 'gz'))
- treat_start: int32 [8192], P(('gx', 'gy', 'gz')), may hold values from 1024 to 4096
- loading_init: float32 [64, 8192], P(None, ('gx', 'gy', 'gz'))
- factor_init: float32 [64, 4096], P(None, ('gx', 'gy', 'gz'))
- unit_init: float32 [8192], P(('gx', 'gy', 'gz'))
- day_init: float32 [4096], replicated
Outputs:
- loading_out: float32 [64, 8192], P(None, ('gx', 'gy', 'gz'))
- factor_out: float32 [64, 4096], P(None, ('gx', 'gy', 'gz'))
- unit_out: float32 [8192], P(('gx', 'gy', 'gz'))
- day_out: float32 [4096], replicated
The draws below stay inside these ranges and needn't reach their ends.
Inputs may be any that keep to these rules, and one draw needn't show every extreme that they name: A unit is treated from day treat_start on; 4096 means never treated.
All inputs are finite; a program needn't handle non-finite values.
Results may differ from the reference program's by a relative error of at most 0.0001.
Values sent between devices are 32-bit elements; how exact they have to be, the bound alone decides.
A program may use at most 64 MiB of HBM per device.

```python
import jax
import jax.numpy as jnp
from jax import lax

RANK = 64
DAYS = 4096
SWEEPS = 2
UNITS = 8192


def truth_parts(key):
    keys = jax.random.split(jax.random.fold_in(key, 7), 4)
    loading_true = jax.random.normal(keys[0], (UNITS, RANK), jnp.float32)
    factor_true = jax.random.normal(keys[1], (RANK, DAYS), jnp.float32) * RANK ** (-0.5)
    unit_true = jax.random.normal(keys[2], (UNITS,), jnp.float32)
    day_true = 0.5 * jax.random.normal(keys[3], (DAYS,), jnp.float32)
    return (loading_true, factor_true, unit_true, day_true)


def draw_panel(key, part):
    loading_true, factor_true, unit_true, day_true = truth_parts(key)
    keys = jax.random.split(jax.random.fold_in(key, 11), 2)
    rising = 1.0 + 2.0 * jnp.arange(UNITS, dtype=jnp.float32) / max(UNITS - 1, 1)
    spread = jnp.exp(jax.random.uniform(keys[0], (UNITS,), jnp.float32, -1.15, 1.15))
    scales = 0.3 * rising * spread
    noise = jax.random.normal(keys[1], (UNITS, DAYS), jnp.float32)
    signal = jnp.dot(loading_true, factor_true, precision=lax.Precision.HIGHEST)
    return unit_true[:, None] + day_true[None, :] + signal + scales[:, None] * noise


def draw_loading_init(key, part):
    loading_true = truth_parts(key)[0]
    noise = jax.random.normal(jax.random.fold_in(key, 21), (UNITS, RANK), jnp.float32)
    return (loading_true + 0.5 * noise).T


def draw_factor_init(key, part):
    factor_true = truth_parts(key)[1]
    noise = jax.random.normal(jax.random.fold_in(key, 31), (RANK, DAYS), jnp.float32)
    return factor_true + 0.5 * RANK ** (-0.5) * noise


def draw_unit_init(key, part):
    unit_true = truth_parts(key)[2]
    return unit_true + 0.3 * jax.random.normal(jax.random.fold_in(key, 41), (UNITS,), jnp.float32)


def draw_day_init(key, part):
    day_true = truth_parts(key)[3]
    return day_true + 0.3 * jax.random.normal(jax.random.fold_in(key, 51), (DAYS,), jnp.float32)


def place_ends(result, rng, low, top_value):
    index_at = [jax.random.randint(jax.random.fold_in(rng, axis), (), 0, length) for axis, length in enumerate(result.shape)]
    widest = result.shape.index(max(result.shape))
    next_to = index_at[:widest] + [(index_at[widest] + 1) % result.shape[widest]] + index_at[widest + 1:]
    return result.at[tuple(index_at)].set(low).at[tuple(next_to)].set(top_value)


def setup_inputs(seed: int = 0) -> dict:
    streams_of = jax.random.split(jax.random.key(seed), 7)
    panel = draw_panel(jax.random.fold_in(streams_of[6], 71), 0)
    treat_start = place_ends(jax.random.randint(streams_of[1], (UNITS,), DAYS // 4, DAYS + 1), jax.random.fold_in(streams_of[1], 1), DAYS // 4, DAYS).astype(jnp.int32)
    loading_init = draw_loading_init(jax.random.fold_in(streams_of[6], 71), 0)
    factor_init = draw_factor_init(jax.random.fold_in(streams_of[6], 71), 0)
    unit_init = draw_unit_init(jax.random.fold_in(streams_of[6], 71), 0)
    day_init = draw_day_init(jax.random.fold_in(streams_of[6], 71), 0)
    return {"panel": panel, "treat_start": treat_start, "loading_init": loading_init, "factor_init": factor_init, "unit_init": unit_init, "day_init": day_init}


RIDGE = 1.0

def solve_spd(matrix, right):
    lower = jnp.linalg.cholesky(matrix)
    middle = lax.linalg.triangular_solve(lower, right, left_side=True, lower=True)
    return lax.linalg.triangular_solve(lower, middle, left_side=True, lower=True, transpose_a=True)

def reference(panel, treat_start, loading_init, factor_init, unit_init, day_init):
    loading = loading_init
    factors = factor_init
    unit_eff = unit_init
    day_eff = day_init
    ridge_eye = jnp.eye(RANK, dtype=jnp.float32) * RIDGE
    observed = lax.broadcasted_iota(jnp.int32, (UNITS, DAYS), 1) < treat_start[:, None]
    for sweep_index in range(SWEEPS):
        fitted = lax.dot_general(loading.astype(jnp.float32), factors.astype(jnp.float32), (((0,), (0,)), ((), ())), precision=lax.Precision.HIGHEST, preferred_element_type=jnp.float32)
        imputed = jnp.where(observed, panel, unit_eff[:, None] + day_eff[None, :] + fitted)
        without = imputed - fitted
        day_sums = jnp.sum(without, 0)
        row_sums = jnp.sum(without, 1)
        grand = jnp.sum(day_sums) / (UNITS * DAYS)
        day_eff = day_sums / UNITS - grand
        unit_eff = row_sums / DAYS - grand
        resid = imputed - unit_eff[:, None] - day_eff[None, :]
        unit_gram = jnp.dot(loading, loading.T, precision=lax.Precision.HIGHEST)
        weighted = jnp.dot(loading, resid, precision=lax.Precision.HIGHEST)
        factors = solve_spd(unit_gram + ridge_eye, weighted)
        factor_gram = jnp.dot(factors, factors.T, precision=lax.Precision.HIGHEST)
        projected = lax.dot_general(factors.astype(jnp.float32), resid.astype(jnp.float32), (((1,), (1,)), ((), ())), precision=lax.Precision.HIGHEST, preferred_element_type=jnp.float32)
        loading = solve_spd(factor_gram + ridge_eye, projected)
    return (loading, factors, unit_eff, day_eff)
```

```python
import functools

import jax
import jax.numpy as jnp
from jax import lax
from jax.experimental import pallas as pl
from jax.experimental.pallas import tpu as pltpu
from jax.sharding import PartitionSpec as P

SWEEPS = 2
RIDGE = 1.0
AXES = ("gx", "gy", "gz")
MESH = pl.DeviceIdType.MESH
VMEM = pl.BlockSpec(memory_space=pltpu.VMEM)


def peers(shape):
    here = {axis: lax.axis_index(axis) for axis in AXES}
    found = {}
    for axis in AXES:
        found[axis] = []
        for step in range(1, shape[axis]):
            there = dict(here)
            there[axis] = lax.rem(here[axis] + step, shape[axis])
            found[axis].append((step, there[axis], tuple(there[name] for name in AXES)))
    return here, found


def meet(found):
    barrier = pltpu.get_barrier_semaphore()
    count = 0
    for axis in AXES:
        for _, _, device in found[axis]:
            pl.semaphore_signal(barrier, inc=1, device_id=device, device_id_type=MESH)
            count += 1
    pl.semaphore_wait(barrier, count)


def spread(out_ref, here, found, send, recv, base):
    index = base
    for depth, axis in ((3, "gx"), (2, "gy"), (1, "gz")):
        at = (here["gz"], here["gy"], here["gx"])[:depth]
        mine = out_ref.at[at]
        copies = []
        for _, _, device in found[axis]:
            copies.append(pltpu.make_async_remote_copy(
                mine, mine, send.at[index], recv.at[index], device_id=device, device_id_type=MESH))
            index += 1
        for copy in copies:
            copy.start()
        for copy in copies:
            copy.wait()


def gather_kernel(shape, own_ref, out_ref, send, recv, local):
    here, found = peers(shape)
    copy = pltpu.make_async_copy(own_ref, out_ref.at[here["gz"], here["gy"], here["gx"]], local)
    copy.start()
    meet(found)
    copy.wait()
    spread(out_ref, here, found, send, recv, 0)


def reduce_kernel(shape, part_ref, out_ref, hold_z, hold_y, hold_x, sum_z, sum_y, send, recv):
    here, found = peers(shape)
    meet(found)
    source = part_ref
    index = 0
    for axis, hold, total in (("gz", hold_z, sum_z), ("gy", hold_y, sum_y), ("gx", hold_x, None)):
        copies = []
        for step, there, device in found[axis]:
            copies.append(pltpu.make_async_remote_copy(
                source.at[there], hold.at[step - 1], send.at[index], recv.at[index],
                device_id=device, device_id_type=MESH))
            index += 1
        for copy in copies:
            copy.start()
        for copy in copies:
            copy.wait()
        value = source[here[axis]]
        for slot in range(len(copies)):
            value = value + hold[slot]
        if total is None:
            out_ref[here["gz"], here["gy"], here["gx"]] = value
        else:
            total[...] = value
            source = total
    spread(out_ref, here, found, send, recv, index)


def links(shape):
    return sum(shape[axis] - 1 for axis in AXES)


def gather(shape, own):
    sizes = (shape["gz"], shape["gy"], shape["gx"])
    count = links(shape)
    return pl.pallas_call(
        functools.partial(gather_kernel, shape),
        out_shape=jax.ShapeDtypeStruct(sizes + own.shape, own.dtype),
        in_specs=[VMEM],
        out_specs=VMEM,
        scratch_shapes=[
            pltpu.SemaphoreType.DMA((count,)), pltpu.SemaphoreType.DMA((count,)), pltpu.SemaphoreType.DMA(()),
        ],
        compiler_params=pltpu.CompilerParams(collective_id=0, has_side_effects=True),
        name="gather_days",
    )(own)


def reduce_all(shape, part):
    z, y, x = shape["gz"], shape["gy"], shape["gx"]
    tiles = part.shape[0]
    block = (tiles // (z * y * x),) + part.shape[1:]
    count = 2 * links(shape)
    f32 = jnp.float32
    total = pl.pallas_call(
        functools.partial(reduce_kernel, shape),
        out_shape=jax.ShapeDtypeStruct((z, y, x) + block, f32),
        in_specs=[VMEM],
        out_specs=VMEM,
        scratch_shapes=[
            pltpu.VMEM((z - 1, y, x) + block, f32),
            pltpu.VMEM((y - 1, x) + block, f32),
            pltpu.VMEM((x - 1,) + block, f32),
            pltpu.VMEM((y, x) + block, f32),
            pltpu.VMEM((x,) + block, f32),
            pltpu.SemaphoreType.DMA((count,)),
            pltpu.SemaphoreType.DMA((count,)),
        ],
        compiler_params=pltpu.CompilerParams(collective_id=1, has_side_effects=True),
        name="reduce_all",
    )(part.reshape((z, y, x) + block))
    return total.reshape(part.shape)


def solve_spd(matrix, right):
    lower = jnp.linalg.cholesky(matrix)
    middle = lax.linalg.triangular_solve(lower, right, left_side=True, lower=True)
    return lax.linalg.triangular_solve(lower, middle, left_side=True, lower=True, transpose_a=True)


def dot(left, right, at):
    return lax.dot_general(
        left, right, ((at[:1], at[1:]), ((), ())), precision=lax.Precision.HIGH, preferred_element_type=jnp.float32)


def body(shape, panel, treat_start, loading_init, factor_init, unit_init, day_init):
    unit_rows, total_days = panel.shape
    devices = shape["gx"] * shape["gy"] * shape["gz"]
    all_units = unit_rows * devices
    rank, slice_days = factor_init.shape
    lanes = 128
    across = total_days // lanes
    gram_rows = -(-rank * rank // total_days)
    rows = -(-(rank + gram_rows + 2) // 8) * 8
    while (rows // 8 * across) % devices:
        rows += 8
    ridge_eye = jnp.eye(rank, dtype=jnp.float32) * RIDGE
    observed = lax.broadcasted_iota(jnp.int32, (unit_rows, total_days), 1) < treat_start[:, None]
    loading, unit_eff, day_eff = loading_init, unit_init, day_init
    factors = gather(shape, factor_init).transpose(3, 2, 1, 0, 4).reshape(rank, total_days)
    for _ in range(SWEEPS):
        fitted = dot(loading, factors, (0, 0))
        imputed = jnp.where(observed, panel, unit_eff[:, None] + day_eff[None, :] + fitted)
        without = imputed - fitted
        day_part = jnp.sum(without, 0)
        row_mean = jnp.sum(without, 1) / total_days
        centred = imputed - row_mean[:, None]
        weighted = dot(loading, centred, (1, 0))
        gram = dot(loading, loading, (1, 1)).reshape(-1)
        gram = jnp.pad(gram, (0, gram_rows * total_days - gram.size)).reshape(gram_rows, total_days)
        load_sum = jnp.pad(jnp.sum(loading, 1), (0, total_days - rank))
        part = jnp.concatenate([weighted, day_part[None], load_sum[None], gram], 0)
        part = jnp.pad(part, ((0, rows - part.shape[0]), (0, 0)))
        part = part.reshape(rows // 8, 8, across, lanes).transpose(0, 2, 1, 3).reshape(-1, 8, lanes)
        total = reduce_all(shape, part)
        total = total.reshape(rows // 8, across, 8, lanes).transpose(0, 2, 1, 3).reshape(rows, total_days)
        weighted = total[:rank]
        day_sums = total[rank]
        load_sum = total[rank + 1, :rank]
        gram = total[rank + 2:rank + 2 + gram_rows].reshape(-1)[:rank * rank].reshape(rank, rank)
        grand = jnp.sum(day_sums) / (all_units * total_days)
        day_eff = day_sums / all_units - grand
        unit_eff = row_mean - grand
        shift = (grand - day_eff)[None, :]
        resid = centred + shift
        factors = solve_spd(gram + ridge_eye, weighted + load_sum[:, None] * shift)
        loading = solve_spd(dot(factors, factors, (1, 1)) + ridge_eye, dot(factors, resid, (1, 1)))
    owned = lax.dynamic_slice_in_dim(factors, lax.axis_index(AXES) * slice_days, slice_days, 1)
    return (loading, owned, unit_eff, day_eff)


def solution(mesh):
    return jax.shard_map(
        functools.partial(body, dict(mesh.shape)),
        mesh=mesh,
        in_specs=(P(AXES, None), P(AXES), P(None, AXES), P(None, AXES), P(AXES), P()),
        out_specs=(P(None, AXES), P(None, AXES), P(AXES), P()),
        check_vma=False,
    )
```

```python
import functools

import jax
import jax.numpy as jnp
from jax import lax
from jax.experimental import pallas as pl
from jax.experimental.pallas import tpu as pltpu
from jax.sharding import PartitionSpec as P

SWEEPS = 2
RIDGE = 1.0
AXES = ("gx", "gy", "gz")
MESH = pl.DeviceIdType.MESH
VMEM = pl.BlockSpec(memory_space=pltpu.VMEM)


def peers(shape):
    here = {axis: lax.axis_index(axis) for axis in AXES}
    found = {}
    for axis in AXES:
        found[axis] = []
        for step in range(1, shape[axis]):
            there = dict(here)
            there[axis] = lax.rem(here[axis] + step, shape[axis])
            found[axis].append((step, there[axis], tuple(there[name] for name in AXES)))
    return here, found


def meet(found):
    barrier = pltpu.get_barrier_semaphore()
    count = 0
    for axis in AXES:
        for _, _, device in found[axis]:
            pl.semaphore_signal(barrier, inc=1, device_id=device, device_id_type=MESH)
            count += 1
    pl.semaphore_wait(barrier, count)


def spread(out_ref, here, found, send, recv, base):
    index = base
    for depth, axis in ((3, "gx"), (2, "gy"), (1, "gz")):
        at = (here["gz"], here["gy"], here["gx"])[:depth]
        mine = out_ref.at[at]
        copies = []
        for _, _, device in found[axis]:
            copies.append(pltpu.make_async_remote_copy(
                mine, mine, send.at[index], recv.at[index], device_id=device, device_id_type=MESH))
            index += 1
        for copy in copies:
            copy.start()
        for copy in copies:
            copy.wait()


def gather_kernel(shape, own_ref, out_ref, send, recv, local):
    here, found = peers(shape)
    copy = pltpu.make_async_copy(own_ref, out_ref.at[here["gz"], here["gy"], here["gx"]], local)
    copy.start()
    meet(found)
    copy.wait()
    spread(out_ref, here, found, send, recv, 0)


def reduce_kernel(shape, part_ref, out_ref, hold_z, hold_y, hold_x, sum_z, sum_y, send, recv):
    here, found = peers(shape)
    meet(found)
    source = part_ref
    index = 0
    for axis, hold, total in (("gz", hold_z, sum_z), ("gy", hold_y, sum_y), ("gx", hold_x, None)):
        copies = []
        for step, there, device in found[axis]:
            copies.append(pltpu.make_async_remote_copy(
                source.at[there], hold.at[step - 1], send.at[index], recv.at[index],
                device_id=device, device_id_type=MESH))
            index += 1
        for copy in copies:
            copy.start()
        for copy in copies:
            copy.wait()
        value = source[here[axis]]
        for slot in range(len(copies)):
            value = value + hold[slot]
        if total is None:
            out_ref[here["gz"], here["gy"], here["gx"]] = value
        else:
            total[...] = value
            source = total
    spread(out_ref, here, found, send, recv, index)


def links(shape):
    return sum(shape[axis] - 1 for axis in AXES)


def gather(shape, own):
    sizes = (shape["gz"], shape["gy"], shape["gx"])
    count = links(shape)
    return pl.pallas_call(
        functools.partial(gather_kernel, shape),
        out_shape=jax.ShapeDtypeStruct(sizes + own.shape, own.dtype),
        in_specs=[VMEM],
        out_specs=VMEM,
        scratch_shapes=[
            pltpu.SemaphoreType.DMA((count,)), pltpu.SemaphoreType.DMA((count,)), pltpu.SemaphoreType.DMA(()),
        ],
        compiler_params=pltpu.CompilerParams(collective_id=0, has_side_effects=True),
        name="gather_days",
    )(own)


def reduce_all(shape, part):
    z, y, x = shape["gz"], shape["gy"], shape["gx"]
    tiles = part.shape[0]
    block = (tiles // (z * y * x),) + part.shape[1:]
    count = 2 * links(shape)
    f32 = jnp.float32
    total = pl.pallas_call(
        functools.partial(reduce_kernel, shape),
        out_shape=jax.ShapeDtypeStruct((z, y, x) + block, f32),
        in_specs=[VMEM],
        out_specs=VMEM,
        scratch_shapes=[
            pltpu.VMEM((z - 1, y, x) + block, f32),
            pltpu.VMEM((y - 1, x) + block, f32),
            pltpu.VMEM((x - 1,) + block, f32),
            pltpu.VMEM((y, x) + block, f32),
            pltpu.VMEM((x,) + block, f32),
            pltpu.SemaphoreType.DMA((count,)),
            pltpu.SemaphoreType.DMA((count,)),
        ],
        compiler_params=pltpu.CompilerParams(collective_id=1, has_side_effects=True),
        name="reduce_all",
    )(part.reshape((z, y, x) + block))
    return total.reshape(part.shape)


def halves(value):
    high = value.astype(jnp.bfloat16)
    return high, (value - high.astype(jnp.float32)).astype(jnp.bfloat16)


def mul(left, right, at):
    return lax.dot_general(left, right, ((at[:1], at[1:]), ((), ())), preferred_element_type=jnp.float32)


def wide_left(value):
    high, low = halves(value)
    return jnp.concatenate([high, high, low], 1)


def wide_right(value):
    high, low = halves(value)
    return jnp.concatenate([high, low, high], 0)


def tall_dot(left, right, at):
    rows = left.shape[0]
    left_high, left_low = halves(left)
    right_high, right_low = halves(right)
    both = mul(jnp.concatenate([left_high, left_low], 0), right_high, (1, at))
    return both[:rows] + both[rows:] + mul(left_high, right_low, (1, at))


def invert(work):
    rank = work.shape[0]
    row_at = lax.broadcasted_iota(jnp.int32, work.shape, 0)
    for k in range(rank):
        pivot_row = work[k:k + 1, :] * (1.0 / work[k:k + 1, k:k + 1])
        work = jnp.where(row_at == k, pivot_row, work - work[:, k:k + 1] * pivot_row)
    return work[:, rank:]


def with_identity(matrix):
    rank = matrix.shape[0]
    eye = jnp.where(
        lax.broadcasted_iota(jnp.int32, (rank, rank), 0) == lax.broadcasted_iota(jnp.int32, (rank, rank), 1), 1.0, 0.0)
    return jnp.concatenate([matrix + RIDGE * eye, eye], 1)


def impute_kernel(width, panel_ref, treat_ref, load_ref, fac_ref, unit_ref, day_ref, part_ref, cent_ref, mean_ref):
    units, days = panel_ref.shape
    rank = load_ref.shape[0]
    lanes = part_ref.shape[2]
    across = days // lanes
    each = width // lanes
    extra = rank // 8 * across
    per = -(-rank // across)
    load = load_ref[...]
    turned = load.T
    load_wide = wide_left(turned)
    part_ref[extra:] = jnp.zeros((part_ref.shape[0] - extra,) + part_ref.shape[1:], jnp.float32)

    def first(tile, total):
        start = pl.multiple_of(tile * width, width)
        cols = pl.ds(start, width)
        fitted = mul(load_wide, wide_right(fac_ref[:, cols]), (1, 0))
        day = lax.broadcasted_iota(jnp.int32, (units, width), 1) + start
        imputed = jnp.where(day < treat_ref[...], panel_ref[:, cols], unit_ref[...] + day_ref[:, cols] + fitted)
        cent_ref[:, cols] = imputed
        without = imputed - fitted
        sums = jnp.sum(without, 0, keepdims=True)
        for c in range(each):
            span = slice(c * lanes, (c + 1) * lanes)
            part_ref[extra + tile * each + c, 0:1, :] = sums[:, span]
            total = total + without[:, span]
        return total

    total = lax.fori_loop(0, days // width, first, jnp.zeros((units, lanes), jnp.float32))
    mean = jnp.sum(total, 1, keepdims=True) / days
    mean_ref[...] = mean

    def second(tile, _):
        cols = pl.ds(pl.multiple_of(tile * width, width), width)
        centred = cent_ref[:, cols] - mean
        cent_ref[:, cols] = centred
        weighted = tall_dot(load, centred, 0)
        for r in range(rank // 8):
            for c in range(each):
                part_ref[r * across + tile * each + c] = weighted[r * 8:r * 8 + 8, c * lanes:(c + 1) * lanes]
        return 0

    lax.fori_loop(0, days // width, second, 0)
    gram = tall_dot(load, load, 1)
    part_ref[extra, 1:2, 0:rank] = jnp.sum(turned, 0, keepdims=True)
    for c in range(-(-rank // per)):
        part_ref[extra + c, 2:2 + per, 0:rank] = gram[c * per:(c + 1) * per]


def solve_kernel(width, devices, total_ref, cent_ref, mean_ref, load_ref, fac_ref, unit_ref, day_ref, gram, shift):
    units, days = cent_ref.shape
    rank = load_ref.shape[0]
    lanes = total_ref.shape[2]
    across = days // lanes
    each = width // lanes
    extra = rank // 8 * across
    per = -(-rank // across)
    for c in range(across):
        shift[0:1, c * lanes:(c + 1) * lanes] = total_ref[extra + c, 0:1, :]
    for c in range(-(-rank // per)):
        gram[c * per:(c + 1) * per, :] = total_ref[extra + c, 2:2 + per, :]
    sums = shift[...]
    grand = jnp.sum(sums, 1, keepdims=True) / (units * devices * days)
    day_eff = sums / (units * devices) - grand
    day_ref[...] = day_eff
    shift[...] = grand - day_eff
    unit_ref[...] = mean_ref[...] - grand
    inverse = wide_left(invert(with_identity(gram[:, 0:rank])))
    same = lax.broadcasted_iota(jnp.int32, (rank, rank), 0) == lax.broadcasted_iota(jnp.int32, (rank, rank), 1)
    load_sum = jnp.sum(jnp.where(same, total_ref[extra, 1:2, 0:rank], 0.0), 1, keepdims=True)

    def step(tile, carry):
        square, projected = carry
        cols = pl.ds(pl.multiple_of(tile * width, width), width)
        weighted = jnp.concatenate([
            jnp.concatenate([total_ref[r * across + tile * each + c] for c in range(each)], 1)
            for r in range(rank // 8)], 0)
        moved = shift[:, cols]
        factors = mul(inverse, wide_right(weighted + load_sum * moved), (1, 0))
        fac_ref[:, cols] = factors
        square = square + tall_dot(factors, factors, 1)
        projected = projected + tall_dot(factors, cent_ref[:, cols] + moved, 1)
        return square, projected

    square, projected = lax.fori_loop(
        0, days // width, step, (jnp.zeros((rank, rank), jnp.float32), jnp.zeros((rank, units), jnp.float32)))
    load_ref[...] = mul(wide_left(invert(with_identity(square))), wide_right(projected), (1, 0))


def body(shape, panel, treat_start, loading_init, factor_init, unit_init, day_init):
    units, days = panel.shape
    devices = shape["gx"] * shape["gy"] * shape["gz"]
    rank, slice_days = factor_init.shape
    lanes = 128
    tiles = (rank // 8 + 1) * (days // lanes)
    tiles = -(-tiles // devices) * devices
    width = min(512, days)
    f32 = jnp.float32

    def array(*sizes):
        return jax.ShapeDtypeStruct(sizes, f32)

    impute = pl.pallas_call(
        functools.partial(impute_kernel, width),
        out_shape=(array(tiles, 8, lanes), array(units, days), array(units, 1)),
        in_specs=[VMEM] * 6,
        out_specs=(VMEM,) * 3,
        name="impute",
    )
    solve = pl.pallas_call(
        functools.partial(solve_kernel, width, devices),
        out_shape=(array(rank, units), array(rank, days), array(units, 1), array(1, days)),
        in_specs=[VMEM] * 3,
        out_specs=(VMEM,) * 4,
        scratch_shapes=[pltpu.VMEM((rank, lanes), f32), pltpu.VMEM((1, days), f32)],
        name="solve",
    )
    treat = treat_start[:, None]
    loading, unit_eff, day_eff = loading_init, unit_init[:, None], day_init[None, :]
    factors = gather(shape, factor_init).transpose(3, 2, 1, 0, 4).reshape(rank, days)
    for _ in range(SWEEPS):
        part, centred, mean = impute(panel, treat, loading, factors, unit_eff, day_eff)
        loading, factors, unit_eff, day_eff = solve(reduce_all(shape, part), centred, mean)
    owned = lax.dynamic_slice_in_dim(factors, lax.axis_index(AXES) * slice_days, slice_days, 1)
    return (loading, owned, unit_eff[:, 0], day_eff[0])


def solution(mesh):
    return jax.shard_map(
        functools.partial(body, dict(mesh.shape)),
        mesh=mesh,
        in_specs=(P(AXES, None), P(AXES), P(None, AXES), P(None, AXES), P(AXES), P()),
        out_specs=(P(None, AXES), P(None, AXES), P(AXES), P()),
        check_vma=False,
    )
```

```python
import functools

import jax
import jax.numpy as jnp
from jax import lax
from jax.experimental import pallas as pl
from jax.experimental.pallas import tpu as pltpu
from jax.sharding import PartitionSpec as P

SWEEPS = 2
RIDGE = 1.0
GATHER_PIECES = 2
REDUCE_PIECES = 3
AXES = ("gx", "gy", "gz")
MESH = pl.DeviceIdType.MESH
VMEM = pl.BlockSpec(memory_space=pltpu.VMEM)


def peers(shape):
    here = {axis: lax.axis_index(axis) for axis in AXES}
    found = {}
    for axis in AXES:
        found[axis] = []
        for step in range(1, shape[axis]):
            there = dict(here)
            there[axis] = lax.rem(here[axis] + step, shape[axis])
            found[axis].append((step, there[axis], tuple(there[name] for name in AXES)))
    return here, found


def meet(found):
    barrier = pltpu.get_barrier_semaphore()
    count = 0
    for axis in AXES:
        for _, _, device in found[axis]:
            pl.semaphore_signal(barrier, inc=1, device_id=device, device_id_type=MESH)
            count += 1
    pl.semaphore_wait(barrier, count)


def send_all(found, source, target, send, recv, base):
    copies = []
    for slot, (step, there, device) in enumerate(found):
        copies.append(pltpu.make_async_remote_copy(
            source(step, there), target(step), send.at[base + slot], recv.at[base + slot],
            device_id=device, device_id_type=MESH))
    for copy in copies:
        copy.start()
    return copies


def finish(copies):
    for copy in copies:
        copy.wait()


def spread(block, place, found, send, recv, base):
    mine = block.at[place]
    return send_all(found, lambda step, there: mine, lambda step: mine, send, recv, base)


def gather_kernel(shape, own_ref, out_ref, blocks, send, recv, local):
    here, found = peers(shape)
    z, y, x = here["gz"], here["gy"], here["gx"]
    pieces, rows = blocks.shape[0], blocks.shape[4]
    width = own_ref.shape[1]
    starts = []
    for p in range(pieces):
        starts.append(pltpu.make_async_copy(own_ref.at[p * rows:(p + 1) * rows], blocks.at[p, z, y, x], local.at[p]))
        starts[p].start()
    meet(found)
    moving = [[copy] for copy in starts]
    index = 0
    for axis, place in (("gx", (z, y, x)), ("gy", (z, y)), ("gz", (z,))):
        for p in range(pieces):
            finish(moving[p])
            moving[p] = spread(blocks.at[p], place, found[axis], send, recv, index)
            index += len(found[axis])
    for p in range(pieces):
        finish(moving[p])
        flat = 0
        for x in range(shape["gx"]):
            for y in range(shape["gy"]):
                for z in range(shape["gz"]):
                    out_ref[p * rows:(p + 1) * rows, flat * width:(flat + 1) * width] = blocks[p, z, y, x]
                    flat += 1


def reduce_kernel(shape, part_ref, out_ref, hold_z, hold_y, hold_x, sum_z, sum_y, send, recv):
    here, found = peers(shape)
    z, y, x = here["gz"], here["gy"], here["gx"]
    pieces = part_ref.shape[0]
    meet(found)
    index = 0
    moving = [[] for _ in range(pieces)]
    for axis, source, hold in (("gz", part_ref, hold_z), ("gy", sum_z, hold_y), ("gx", sum_y, hold_x)):
        for p in range(pieces):
            if axis == "gy":
                finish(moving[p])
                value = part_ref[p, z]
                for slot in range(shape["gz"] - 1):
                    value = value + hold_z[p, slot]
                sum_z[p] = value
            if axis == "gx":
                finish(moving[p])
                value = sum_z[p, y]
                for slot in range(shape["gy"] - 1):
                    value = value + hold_y[p, slot]
                sum_y[p] = value
            moving[p] = send_all(
                found[axis], lambda step, there: source.at[p, there], lambda step: hold.at[p, step - 1],
                send, recv, index)
            index += len(found[axis])
    for axis, place in (("gx", (z, y, x)), ("gy", (z, y)), ("gz", (z,))):
        for p in range(pieces):
            finish(moving[p])
            if axis == "gx":
                value = sum_y[p, x]
                for slot in range(shape["gx"] - 1):
                    value = value + hold_x[p, slot]
                out_ref[p, z, y, x] = value
            moving[p] = spread(out_ref.at[p], place, found[axis], send, recv, index)
            index += len(found[axis])
    for p in range(pieces):
        finish(moving[p])


def links(shape):
    return sum(shape[axis] - 1 for axis in AXES)


def gather(shape, own):
    pieces = GATHER_PIECES
    rows, width = own.shape
    devices = shape["gx"] * shape["gy"] * shape["gz"]
    count = pieces * links(shape)
    return pl.pallas_call(
        functools.partial(gather_kernel, shape),
        out_shape=jax.ShapeDtypeStruct((rows, devices * width), own.dtype),
        in_specs=[VMEM],
        out_specs=VMEM,
        scratch_shapes=[
            pltpu.VMEM((pieces, shape["gz"], shape["gy"], shape["gx"], rows // pieces, width), own.dtype),
            pltpu.SemaphoreType.DMA((count,)), pltpu.SemaphoreType.DMA((count,)), pltpu.SemaphoreType.DMA((pieces,)),
        ],
        compiler_params=pltpu.CompilerParams(collective_id=0, has_side_effects=True),
        name="gather_days",
    )(own)


def reduce_all(shape, part):
    z, y, x = shape["gz"], shape["gy"], shape["gx"]
    pieces = REDUCE_PIECES
    tiles = part.shape[0]
    block = (tiles // (pieces * z * y * x),) + part.shape[1:]
    count = 2 * pieces * links(shape)
    f32 = jnp.float32
    total = pl.pallas_call(
        functools.partial(reduce_kernel, shape),
        out_shape=jax.ShapeDtypeStruct((pieces, z, y, x) + block, f32),
        in_specs=[VMEM],
        out_specs=VMEM,
        scratch_shapes=[
            pltpu.VMEM((pieces, z - 1, y, x) + block, f32),
            pltpu.VMEM((pieces, y - 1, x) + block, f32),
            pltpu.VMEM((pieces, x - 1) + block, f32),
            pltpu.VMEM((pieces, y, x) + block, f32),
            pltpu.VMEM((pieces, x) + block, f32),
            pltpu.SemaphoreType.DMA((count,)),
            pltpu.SemaphoreType.DMA((count,)),
        ],
        compiler_params=pltpu.CompilerParams(collective_id=1, has_side_effects=True),
        name="reduce_all",
    )(part.reshape((pieces, z, y, x) + block))
    return total.reshape(part.shape)


def halves(value):
    high = value.astype(jnp.bfloat16)
    return high, (value - high.astype(jnp.float32)).astype(jnp.bfloat16)


def mul(left, right, at):
    return lax.dot_general(left, right, ((at[:1], at[1:]), ((), ())), preferred_element_type=jnp.float32)


def wide_left(value):
    high, low = halves(value)
    return jnp.concatenate([high, high, low], 1)


def wide_right(value):
    high, low = halves(value)
    return jnp.concatenate([high, low, high], 0)


def tall_dot(left, right, at):
    rows = left.shape[0]
    left_high, left_low = halves(left)
    right_high, right_low = halves(right)
    both = mul(jnp.concatenate([left_high, left_low], 0), right_high, (1, at))
    return both[:rows] + both[rows:] + mul(left_high, right_low, (1, at))


def invert(work):
    rank = work.shape[0]
    row_at = lax.broadcasted_iota(jnp.int32, work.shape, 0)
    for k in range(rank):
        pivot_row = work[k:k + 1, :] * (1.0 / work[k:k + 1, k:k + 1])
        work = jnp.where(row_at == k, pivot_row, work - work[:, k:k + 1] * pivot_row)
    return work[:, rank:]


def with_identity(matrix):
    rank = matrix.shape[0]
    eye = jnp.where(
        lax.broadcasted_iota(jnp.int32, (rank, rank), 0) == lax.broadcasted_iota(jnp.int32, (rank, rank), 1), 1.0, 0.0)
    return jnp.concatenate([matrix + RIDGE * eye, eye], 1)


def impute_kernel(width, panel_ref, treat_ref, load_ref, fac_ref, unit_ref, day_ref, part_ref, cent_ref, mean_ref):
    units, days = panel_ref.shape
    rank = load_ref.shape[0]
    lanes = part_ref.shape[2]
    across = days // lanes
    each = width // lanes
    extra = rank // 8 * across
    per = -(-rank // across)
    load = load_ref[...]
    turned = load.T
    load_wide = wide_left(turned)
    part_ref[extra:] = jnp.zeros((part_ref.shape[0] - extra,) + part_ref.shape[1:], jnp.float32)

    def first(tile, total):
        start = pl.multiple_of(tile * width, width)
        cols = pl.ds(start, width)
        fitted = mul(load_wide, wide_right(fac_ref[:, cols]), (1, 0))
        day = lax.broadcasted_iota(jnp.int32, (units, width), 1) + start
        imputed = jnp.where(day < treat_ref[...], panel_ref[:, cols], unit_ref[...] + day_ref[:, cols] + fitted)
        cent_ref[:, cols] = imputed
        without = imputed - fitted
        sums = jnp.sum(without, 0, keepdims=True)
        for c in range(each):
            span = slice(c * lanes, (c + 1) * lanes)
            part_ref[extra + tile * each + c, 0:1, :] = sums[:, span]
            total = total + without[:, span]
        return total

    total = lax.fori_loop(0, days // width, first, jnp.zeros((units, lanes), jnp.float32))
    mean = jnp.sum(total, 1, keepdims=True) / days
    mean_ref[...] = mean

    def second(tile, _):
        cols = pl.ds(pl.multiple_of(tile * width, width), width)
        centred = cent_ref[:, cols] - mean
        cent_ref[:, cols] = centred
        weighted = tall_dot(load, centred, 0)
        for r in range(rank // 8):
            for c in range(each):
                part_ref[r * across + tile * each + c] = weighted[r * 8:r * 8 + 8, c * lanes:(c + 1) * lanes]
        return 0

    lax.fori_loop(0, days // width, second, 0)
    gram = tall_dot(load, load, 1)
    part_ref[extra, 1:2, 0:rank] = jnp.sum(turned, 0, keepdims=True)
    for c in range(-(-rank // per)):
        part_ref[extra + c, 2:2 + per, 0:rank] = gram[c * per:(c + 1) * per]


def solve_kernel(width, devices, total_ref, cent_ref, mean_ref, load_ref, fac_ref, unit_ref, day_ref, gram, shift):
    units, days = cent_ref.shape
    rank = load_ref.shape[0]
    lanes = total_ref.shape[2]
    across = days // lanes
    each = width // lanes
    extra = rank // 8 * across
    per = -(-rank // across)
    for c in range(across):
        shift[0:1, c * lanes:(c + 1) * lanes] = total_ref[extra + c, 0:1, :]
    for c in range(-(-rank // per)):
        gram[c * per:(c + 1) * per, :] = total_ref[extra + c, 2:2 + per, :]
    sums = shift[...]
    grand = jnp.sum(sums, 1, keepdims=True) / (units * devices * days)
    day_eff = sums / (units * devices) - grand
    day_ref[...] = day_eff
    shift[...] = grand - day_eff
    unit_ref[...] = mean_ref[...] - grand
    inverse = wide_left(invert(with_identity(gram[:, 0:rank])))
    same = lax.broadcasted_iota(jnp.int32, (rank, rank), 0) == lax.broadcasted_iota(jnp.int32, (rank, rank), 1)
    load_sum = jnp.sum(jnp.where(same, total_ref[extra, 1:2, 0:rank], 0.0), 1, keepdims=True)

    def step(tile, carry):
        square, projected = carry
        cols = pl.ds(pl.multiple_of(tile * width, width), width)
        weighted = jnp.concatenate([
            jnp.concatenate([total_ref[r * across + tile * each + c] for c in range(each)], 1)
            for r in range(rank // 8)], 0)
        moved = shift[:, cols]
        factors = mul(inverse, wide_right(weighted + load_sum * moved), (1, 0))
        fac_ref[:, cols] = factors
        square = square + tall_dot(factors, factors, 1)
        projected = projected + tall_dot(factors, cent_ref[:, cols] + moved, 1)
        return square, projected

    square, projected = lax.fori_loop(
        0, days // width, step, (jnp.zeros((rank, rank), jnp.float32), jnp.zeros((rank, units), jnp.float32)))
    load_ref[...] = mul(wide_left(invert(with_identity(square))), wide_right(projected), (1, 0))


def body(shape, panel, treat_start, loading_init, factor_init, unit_init, day_init):
    units, days = panel.shape
    devices = shape["gx"] * shape["gy"] * shape["gz"]
    rank, slice_days = factor_init.shape
    lanes = 128
    tiles = (rank // 8 + 1) * (days // lanes)
    tiles = -(-tiles // (REDUCE_PIECES * devices)) * REDUCE_PIECES * devices
    width = min(512, days)
    f32 = jnp.float32

    def array(*sizes):
        return jax.ShapeDtypeStruct(sizes, f32)

    impute = pl.pallas_call(
        functools.partial(impute_kernel, width),
        out_shape=(array(tiles, 8, lanes), array(units, days), array(units, 1)),
        in_specs=[VMEM] * 6,
        out_specs=(VMEM,) * 3,
        name="impute",
    )
    solve = pl.pallas_call(
        functools.partial(solve_kernel, width, devices),
        out_shape=(array(rank, units), array(rank, days), array(units, 1), array(1, days)),
        in_specs=[VMEM] * 3,
        out_specs=(VMEM,) * 4,
        scratch_shapes=[pltpu.VMEM((rank, lanes), f32), pltpu.VMEM((1, days), f32)],
        name="solve",
    )
    treat = treat_start[:, None]
    loading, unit_eff, day_eff = loading_init, unit_init[:, None], day_init[None, :]
    factors = gather(shape, factor_init)
    for _ in range(SWEEPS):
        part, centred, mean = impute(panel, treat, loading, factors, unit_eff, day_eff)
        loading, factors, unit_eff, day_eff = solve(reduce_all(shape, part), centred, mean)
    owned = lax.dynamic_slice_in_dim(factors, lax.axis_index(AXES) * slice_days, slice_days, 1)
    return (loading, owned, unit_eff[:, 0], day_eff[0])


def solution(mesh):
    return jax.shard_map(
        functools.partial(body, dict(mesh.shape)),
        mesh=mesh,
        in_specs=(P(AXES, None), P(AXES), P(None, AXES), P(None, AXES), P(AXES), P()),
        out_specs=(P(None, AXES), P(None, AXES), P(AXES), P()),
        check_vma=False,
    )
```
